32 devices in a mesh: clip: 2 (over x), tm: 16 (over z, y, core).
Axes of the slice: x: 2, y: 2, z: 4, core: 2. Of those that a mesh axis runs over, the one named last changes fastest.
Arguments:
- frames: bfloat16 [64, 1024, 256], P('tm', 'clip'), parts along dimension 1, may hold values from -6 to 6
- gain_one: float32 [256], replicated, may hold values from 0.25 to 1.75
- conv_one: bfloat16 [3, 3, 3, 256, 256], replicated, may hold values from -0.078125 to 0.078125
- gain_two: float32 [256], replicated, may hold values from 0.25 to 1.75
- conv_two: bfloat16 [3, 3, 3, 256, 256], replicated, may hold values from -0.078125 to 0.078125
- out_weight: bfloat16 [256, 256], replicated, may hold values from -0.375 to 0.375
Outputs:
- latent: bfloat16 [64, 1024, 256], P(None, ('clip', 'tm')), parts along dimension 1
The draws below stay inside these ranges and needn't reach their ends.
There are 2 independent parts, one for each index of `clip`. The reference program is written for one: setup_inputs(seed, part) draws one part's arguments, and reference() takes and returns one part's arrays. A program takes and returns all parts, laid end to end along the dimension named above; an argument that names none is the same for every part. Nothing has to cross between parts.
All inputs are finite; a program needn't handle non-finite values.
Results may differ from the reference program's by a relative error of at most 0.0065.
Values may be sent and summed in bfloat16 or wider, within the bound.
No kernel may reach another device: no remote copies, remote signals or barrier semaphores. Data moves between devices by JAX's collectives and lax.ppermute only.
A program may use at most 192 MiB of HBM per device.

```python
import jax
import jax.numpy as jnp
from jax import lax

C = 256
ROWS = 4
COLS = 128
CELLS = 512
FRAMES = 64


def levels(rng, dims, split, low, largest):
    def one(axis_at, shards_of):
        steps = jax.random.uniform(jax.random.fold_in(jax.random.fold_in(rng, 6), axis_at), (shards_of,), jnp.float32, low / len(split), largest / len(split))
        return jnp.repeat(jnp.exp(steps), dims[axis_at] // shards_of).reshape((-1,) + (1,) * (len(dims) - axis_at - 1))

    factor_of = one(*split[0])
    for cut in split[1:]:
        factor_of = factor_of * one(*cut)
    return factor_of


def bell_draw(stream_key, shape, width, limit, cuts=(), kind=jnp.bfloat16):
    values = width * jax.random.normal(stream_key, shape, jnp.float32)
    if cuts:
        values = values * levels(stream_key, shape, cuts, -0.22, 0.18)
    return jnp.clip(values, -limit, limit).astype(kind)


def setup_inputs(seed: int = 0, part: int = 0) -> dict:
    arg_keys = jax.random.split(jax.random.key(seed), 7)
    part_splits = jax.random.split(jax.random.fold_in(arg_keys[6], part), 7)
    return {
        "frames": bell_draw(part_splits[0], (FRAMES, CELLS, C), 1.0, 6.0, ((0, 16),)),
        "gain_one": jnp.clip(1.0 + 0.15 * jax.random.normal(arg_keys[1], (C,), jnp.float32), 0.25, 1.75),
        "conv_one": bell_draw(arg_keys[2], (3, 3, 3, C, C), (27 * C) ** -0.5, 0.078125),
        "gain_two": jnp.clip(1.0 + 0.15 * jax.random.normal(arg_keys[3], (C,), jnp.float32), 0.25, 1.75),
        "conv_two": bell_draw(arg_keys[4], (3, 3, 3, C, C), (27 * C) ** -0.5, 0.078125),
        "out_weight": bell_draw(arg_keys[5], (C, C), C ** -0.5, 0.375),
    }


def norm_act(x, gain):
    values = x.astype(jnp.float32)
    scale = lax.rsqrt(lax.optimization_barrier(jnp.mean(values * values, axis=-1, keepdims=True)) + 1e-06)
    return jax.nn.silu(values * scale * gain).astype(jnp.bfloat16)

def causal_conv(act, kernel):
    frame_count = act.shape[0]
    channels = act.shape[-1]
    grid = act.reshape(frame_count, ROWS, COLS, channels)
    padded = jnp.pad(grid, ((2, 0), (1, 1), (1, 1), (0, 0)))
    total = jnp.zeros((frame_count * ROWS * COLS, channels), jnp.float32)
    for tap_t in range(3):
        for tap_r in range(3):
            for tap_c in range(3):
                slab = padded[tap_t:tap_t + frame_count, tap_r:tap_r + ROWS, tap_c:tap_c + COLS, :]
                total = total + jnp.dot(slab.reshape(-1, channels), kernel[tap_t, tap_r, tap_c], preferred_element_type=jnp.float32)
    return total.reshape(frame_count, ROWS * COLS, channels)

def block(x, gain, kernel):
    act = norm_act(x, gain)
    return (x.astype(jnp.float32) + causal_conv(act, kernel)).astype(jnp.bfloat16)

def reference(frames, gain_one, conv_one, gain_two, conv_two, out_weight):
    first = block(frames, gain_one, conv_one)
    second = block(first, gain_two, conv_two)
    channels = second.shape[-1]
    latent = jnp.dot(second.reshape(-1, channels), out_weight, preferred_element_type=jnp.float32)
    return latent.reshape(second.shape).astype(jnp.bfloat16)
```

```python
import functools

import jax
import jax.numpy as jnp
from jax import lax
from jax.experimental import pallas as pl
from jax.experimental.pallas import tpu as pltpu
from jax.sharding import PartitionSpec as P

ROWS = 4
COLS = 128
HALO = 2


def passed_along(x, axis, by):
    size = lax.axis_size(axis)
    pairs = [(i, i + by) for i in range(size) if 0 <= i + by < size]
    return lax.ppermute(x, axis, pairs)


def norm_act(x, gain):
    values = x.astype(jnp.float32)
    scale = lax.rsqrt(jnp.mean(values * values, axis=-1, keepdims=True) + 1e-06)
    gated = values * scale * gain
    return gated / (1.0 + jnp.exp(-gated))


def conv_body(groups, project, *refs):
    sources = refs[:groups]
    gain_ref, kernel_hbm = refs[groups], refs[groups + 1]
    rest = refs[groups + 2 :]
    if project:
        weight_ref, rest = rest[0], rest[1:]
    out_ref, taps_ref, sum_ref, kernel_ref, sems = rest
    channels = gain_ref.shape[-1]
    order = [(a, b) for b in (1, 0, 2) for a in range(3)]
    copies = {
        (a, b): pltpu.make_async_copy(kernel_hbm.at[a, b], kernel_ref.at[a, b], sems.at[a, b])
        for a, b in order
    }
    for key in order:
        copies[key].start()
    column = lax.broadcasted_iota(jnp.int32, (COLS, channels), 0)
    gain = gain_ref[...]

    for group, source in enumerate(sources):

        def prepare(i, carry, source=source, group=group):
            frame, row = i // ROWS, i % ROWS
            cells = pl.ds(pl.multiple_of(row * COLS, COLS), COLS)
            act = norm_act(source[frame, cells, :], gain)
            left = jnp.where(column == 0, 0.0, pltpu.roll(act, 1, 0))
            right = jnp.where(column == COLS - 1, 0.0, pltpu.roll(act, COLS - 1, 0))
            at = HALO * group + frame
            taps_ref[at, row, :, :channels] = left.astype(jnp.bfloat16)
            taps_ref[at, row, :, channels : 2 * channels] = act.astype(jnp.bfloat16)
            taps_ref[at, row, :, 2 * channels :] = right.astype(jnp.bfloat16)
            return carry

        lax.fori_loop(0, HALO * ROWS, prepare, 0, unroll=2)

    for part in range(groups - 1):
        base = HALO * part
        for a, b in order:
            if part == 0:
                copies[a, b].wait()
            first_in, first_out, count = {1: (0, 0, ROWS), 0: (0, 1, ROWS - 1), 2: (1, 0, ROWS - 1)}[b]
            window = taps_ref[base + a : base + a + HALO, first_in : first_in + count]
            product = jnp.dot(
                window.reshape(HALO * count * COLS, 3 * channels),
                kernel_ref[a, b],
                preferred_element_type=jnp.float32,
            ).reshape(HALO, count * COLS, channels)
            if (a, b) == order[0]:
                sum_ref[...] = product + sources[part + 1][...].astype(jnp.float32)
            else:
                sum_ref[:, first_out * COLS : (first_out + count) * COLS] += product
        block = sum_ref[...].astype(jnp.bfloat16)
        if project:
            block = jnp.dot(
                block.reshape(HALO * ROWS * COLS, channels),
                weight_ref[...],
                preferred_element_type=jnp.float32,
            ).astype(jnp.bfloat16)
            if len(out_ref.shape) == 4:
                owners, _, owned, _ = out_ref.shape
                block = block.reshape(HALO, owners, owned, channels)
                for frame in range(HALO):
                    out_ref[:, base + frame] = block[frame]
            else:
                out_ref[base : base + HALO] = block.reshape(HALO, ROWS * COLS, channels)
        else:
            out_ref[base : base + HALO] = block


def conv_block(sources, gain, kernel, weight=None, owners=None):
    groups = len(sources)
    outcount = HALO * (groups - 1)
    cells, channels = sources[0][0].shape[1:]
    flat_kernel = kernel.reshape(3, 3, 3 * channels, channels)
    whole = lambda *dims: pl.BlockSpec(dims, lambda i: (0,) * len(dims))
    operands = [array for array, _ in sources] + [gain.reshape(1, channels), flat_kernel]
    specs = [
        pl.BlockSpec((HALO, cells, channels), functools.partial(lambda at, i: (at, 0, 0), at))
        for _, at in sources
    ] + [whole(1, channels), pl.BlockSpec(memory_space=pl.ANY)]
    if weight is not None:
        operands.append(weight)
        specs.append(whole(channels, channels))
    if owners is not None:
        shape = (owners, outcount, cells // owners, channels)
    else:
        shape = (outcount, cells, channels)
    flops = 2 * outcount * cells * 27 * channels * channels
    return pl.pallas_call(
        functools.partial(conv_body, groups, weight is not None),
        grid=(1,),
        in_specs=specs,
        out_specs=whole(*shape),
        out_shape=jax.ShapeDtypeStruct(shape, jnp.bfloat16),
        scratch_shapes=[
            pltpu.VMEM((HALO * groups, ROWS, COLS, 3 * channels), jnp.bfloat16),
            pltpu.VMEM((HALO, cells, channels), jnp.float32),
            pltpu.VMEM((3, 3, 3 * channels, channels), jnp.bfloat16),
            pltpu.SemaphoreType.DMA((3, 3)),
        ],
        compiler_params=pltpu.CompilerParams(vmem_limit_bytes=56 * 1024 * 1024),
        cost_estimate=pl.CostEstimate(
            flops=flops, bytes_accessed=27 * channels * channels * 2, transcendentals=0
        ),
    )(*operands)


def body(frames, gain_one, conv_one, gain_two, conv_two, out_weight):
    local_frames, cells, channels = frames.shape
    members = lax.axis_size("tm")
    owned = cells // members
    assert local_frames == 2 * HALO
    earlier = passed_along(frames[-HALO:], "tm", 1)
    late = conv_block([(frames, 0), (frames, 1)], gain_one, conv_one)
    late_earlier = passed_along(late, "tm", 1)
    early = conv_block([(earlier, 0), (frames, 0)], gain_one, conv_one)
    aligned = owned % 16 == 0
    projected = conv_block(
        [(late_earlier, 0), (early, 0), (late, 0)],
        gain_two,
        conv_two,
        out_weight,
        members if aligned else None,
    )
    if aligned:
        latent = lax.all_to_all(projected, "tm", split_axis=0, concat_axis=0, tiled=True)
    else:
        latent = lax.all_to_all(projected, "tm", split_axis=1, concat_axis=0, tiled=True)
    return latent.reshape(members * local_frames, owned, channels)


def solution(mesh):
    placed = (P("tm", "clip", None), P(), P(), P(), P(), P())
    return jax.shard_map(
        body, mesh=mesh, in_specs=placed, out_specs=P(None, ("clip", "tm"), None), check_vma=False
    )
```

```python
import functools

import jax
import jax.numpy as jnp
from jax import lax
from jax.experimental import pallas as pl
from jax.experimental.pallas import tpu as pltpu
from jax.sharding import PartitionSpec as P

ROWS = 4
COLS = 128
HALO = 2
VMEM_LIMIT = 24 * 1024 * 1024


def passed_along(x, axis, by):
    size = lax.axis_size(axis)
    pairs = [(i, i + by) for i in range(size) if 0 <= i + by < size]
    return lax.ppermute(x, axis, pairs)


def norm_act(x, gain):
    values = x.astype(jnp.float32)
    scale = lax.rsqrt(jnp.mean(values * values, axis=-1, keepdims=True) + 1e-06)
    gated = values * scale * gain
    return gated / (1.0 + jnp.exp(-gated))


def conv_body(groups, project, *refs):
    sources = refs[:groups]
    gain_ref, kernel_ref = refs[groups], refs[groups + 1]
    rest = refs[groups + 2 :]
    if project:
        weight_ref, rest = rest[0], rest[1:]
    out_ref, taps_ref, sum_ref = rest
    channels = gain_ref.shape[-1]
    column = lax.broadcasted_iota(jnp.int32, (COLS, channels), 0)
    gain = gain_ref[...]

    for group, source in enumerate(sources):

        def prepare(i, carry, source=source, group=group):
            frame, row = i // ROWS, i % ROWS
            cells = pl.ds(pl.multiple_of(row * COLS, COLS), COLS)
            act = norm_act(source[frame, cells, :], gain)
            left = jnp.where(column == 0, 0.0, pltpu.roll(act, 1, 0))
            right = jnp.where(column == COLS - 1, 0.0, pltpu.roll(act, COLS - 1, 0))
            at = HALO * group + frame
            taps_ref[at, row, :, :channels] = left.astype(jnp.bfloat16)
            taps_ref[at, row, :, channels : 2 * channels] = act.astype(jnp.bfloat16)
            taps_ref[at, row, :, 2 * channels :] = right.astype(jnp.bfloat16)
            return carry

        lax.fori_loop(0, HALO * ROWS, prepare, 0, unroll=4)

    for part in range(groups - 1):
        base = HALO * part
        for row in range(ROWS):
            bs = [b for b in range(3) if 0 <= row + b - 1 < ROWS]
            kern = jnp.concatenate([kernel_ref[a, b] for b in bs for a in range(3)], axis=0)
            win = jnp.concatenate([taps_ref[base + a : base + a + HALO, row + b - 1].reshape(HALO*COLS, 3*channels) for b in bs for a in range(3)], axis=1)
            product = jnp.dot(win, kern, preferred_element_type=jnp.float32).reshape(HALO, COLS, channels)
            at = slice(row * COLS, (row + 1) * COLS)
            sum_ref[:, at] = product + sources[part + 1][:, at, :].astype(jnp.float32)
        block = sum_ref[...].astype(jnp.bfloat16)
        if project:
            block = jnp.dot(
                block.reshape(HALO * ROWS * COLS, channels),
                weight_ref[...],
                preferred_element_type=jnp.float32,
            ).astype(jnp.bfloat16)
            if len(out_ref.shape) == 4:
                owners, _, owned, _ = out_ref.shape
                block = block.reshape(HALO, owners, owned, channels)
                for frame in range(HALO):
                    out_ref[:, base + frame] = block[frame]
            else:
                out_ref[base : base + HALO] = block.reshape(HALO, ROWS * COLS, channels)
        else:
            out_ref[base : base + HALO] = block


def conv_block(sources, gain, kernel, weight=None, owners=None):
    groups = len(sources)
    outcount = HALO * (groups - 1)
    cells, channels = sources[0][0].shape[1:]
    flat_kernel = kernel.reshape(3, 3, 3 * channels, channels)
    whole = lambda *dims: pl.BlockSpec(dims, lambda i: (0,) * len(dims))
    operands = [array for array, _ in sources] + [gain.reshape(1, channels), flat_kernel]
    specs = [
        pl.BlockSpec((HALO, cells, channels), functools.partial(lambda at, i: (at, 0, 0), at))
        for _, at in sources
    ] + [whole(1, channels), whole(3, 3, 3 * channels, channels)]
    if weight is not None:
        operands.append(weight)
        specs.append(whole(channels, channels))
    if owners is not None:
        shape = (owners, outcount, cells // owners, channels)
    else:
        shape = (outcount, cells, channels)
    flops = 2 * outcount * cells * 27 * channels * channels
    return pl.pallas_call(
        functools.partial(conv_body, groups, weight is not None),
        grid=(1,),
        in_specs=specs,
        out_specs=whole(*shape),
        out_shape=jax.ShapeDtypeStruct(shape, jnp.bfloat16),
        scratch_shapes=[
            pltpu.VMEM((HALO * groups, ROWS, COLS, 3 * channels), jnp.bfloat16),
            pltpu.VMEM((HALO, cells, channels), jnp.float32),
        ],
        compiler_params=pltpu.CompilerParams(vmem_limit_bytes=VMEM_LIMIT),
        cost_estimate=pl.CostEstimate(
            flops=flops, bytes_accessed=27 * channels * channels * 2, transcendentals=0
        ),
    )(*operands)


def body(frames, gain_one, conv_one, gain_two, conv_two, out_weight):
    local_frames, cells, channels = frames.shape
    members = lax.axis_size("tm")
    owned = cells // members
    assert local_frames == 2 * HALO
    earlier = passed_along(frames[-HALO:], "tm", 1)
    late = conv_block([(frames, 0), (frames, 1)], gain_one, conv_one)
    late_earlier = passed_along(late, "tm", 1)
    early = conv_block([(earlier, 0), (frames, 0)], gain_one, conv_one)
    aligned = owned % 16 == 0
    projected = conv_block(
        [(late_earlier, 0), (early, 0), (late, 0)],
        gain_two,
        conv_two,
        out_weight,
        members if aligned else None,
    )
    if aligned:
        latent = lax.all_to_all(projected, "tm", split_axis=0, concat_axis=0, tiled=True)
    else:
        latent = lax.all_to_all(projected, "tm", split_axis=1, concat_axis=0, tiled=True)
    return latent.reshape(members * local_frames, owned, channels)


def solution(mesh):
    placed = (P("tm", "clip", None), P(), P(), P(), P(), P())
    return jax.shard_map(
        body, mesh=mesh, in_specs=placed, out_specs=P(None, ("clip", "tm"), None), check_vma=False
    )
```

```python
import functools

import jax
import jax.numpy as jnp
from jax import lax
from jax.experimental import pallas as pl
from jax.experimental.pallas import tpu as pltpu
from jax.sharding import PartitionSpec as P

ROWS = 4
COLS = 128
HALO = 2
VMEM_LIMIT = 24 * 1024 * 1024


def passed_along(x, axis, by):
    size = lax.axis_size(axis)
    pairs = [(i, i + by) for i in range(size) if 0 <= i + by < size]
    return lax.ppermute(x, axis, pairs)


def norm_act(x, gain):
    values = x.astype(jnp.float32)
    scale = lax.rsqrt(jnp.mean(values * values, axis=-1, keepdims=True) + 1e-06)
    gated = values * scale * gain
    return gated / (1.0 + jnp.exp(-gated))


def spread(source, frame, row, gain, taps_ref, at):
    channels = source.shape[-1]
    column = lax.broadcasted_iota(jnp.int32, (COLS, channels), 0)
    cells = pl.ds(pl.multiple_of(row * COLS, COLS), COLS)
    act = norm_act(source[frame, cells, :], gain)
    left = jnp.where(column == 0, 0.0, pltpu.roll(act, 1, 0))
    right = jnp.where(column == COLS - 1, 0.0, pltpu.roll(act, COLS - 1, 0))
    taps_ref[at, row, :, :channels] = left.astype(jnp.bfloat16)
    taps_ref[at, row, :, channels : 2 * channels] = act.astype(jnp.bfloat16)
    taps_ref[at, row, :, 2 * channels :] = right.astype(jnp.bfloat16)


def taps_body(source, gain_ref, taps_ref):
    gain = gain_ref[...]

    def prepare(row, carry):
        spread(source, 0, row, gain, taps_ref, 0)
        return carry

    lax.fori_loop(0, ROWS, prepare, 0, unroll=4)


def taps_of(x, gain):
    frames, cells, channels = x.shape
    return pl.pallas_call(
        taps_body,
        grid=(frames,),
        in_specs=[
            pl.BlockSpec((1, cells, channels), lambda i: (i, 0, 0)),
            pl.BlockSpec((1, channels), lambda i: (0, 0)),
        ],
        out_specs=pl.BlockSpec((1, ROWS, COLS, 3 * channels), lambda i: (i, 0, 0, 0)),
        out_shape=jax.ShapeDtypeStruct((frames, ROWS, COLS, 3 * channels), jnp.bfloat16),
        compiler_params=pltpu.CompilerParams(vmem_limit_bytes=VMEM_LIMIT),
        cost_estimate=pl.CostEstimate(
            flops=20 * frames * cells * channels, bytes_accessed=8 * frames * cells * channels, transcendentals=0
        ),
    )(x, gain.reshape(1, channels))


def conv_body(ready, project, *refs):
    groups = len(ready)
    sources, refs = refs[:groups], list(refs[groups:])
    residuals = [refs.pop(0) if ready[g] else sources[g] for g in range(1, groups)]
    gain_ref, kernel_ref = refs[:2]
    rest = refs[2:]
    if project:
        weight_ref, rest = rest[0], rest[1:]
    out_ref, taps_ref, sum_ref = rest
    channels = gain_ref.shape[-1]
    gain = gain_ref[...]

    for group, source in enumerate(sources):
        if ready[group]:
            continue

        def prepare(i, carry, source=source, group=group):
            frame, row = i // ROWS, i % ROWS
            spread(source, frame, row, gain, taps_ref, HALO * group + frame)
            return carry

        lax.fori_loop(0, HALO * ROWS, prepare, 0, unroll=4)

    def tap(frame, row):
        if ready[frame // HALO]:
            return sources[frame // HALO][frame % HALO, row]
        return taps_ref[frame, row]

    for part in range(groups - 1):
        base = HALO * part
        for row in range(ROWS):
            taps = [(a, b) for b in range(3) if 0 <= row + b - 1 < ROWS for a in range(3)]
            window = jnp.concatenate(
                [
                    jnp.concatenate([tap(base + a + f, row + b - 1) for f in range(HALO)], axis=0)
                    for a, b in taps
                ],
                axis=1,
            )
            product = jnp.dot(
                window,
                jnp.concatenate([kernel_ref[a, b] for a, b in taps], axis=0),
                preferred_element_type=jnp.float32,
            ).reshape(HALO, COLS, channels)
            at = slice(row * COLS, (row + 1) * COLS)
            sum_ref[:, at] = product + residuals[part][:, at, :].astype(jnp.float32)
        block = sum_ref[...].astype(jnp.bfloat16)
        if project:
            block = jnp.dot(
                block.reshape(HALO * ROWS * COLS, channels),
                weight_ref[...],
                preferred_element_type=jnp.float32,
            ).astype(jnp.bfloat16)
            if len(out_ref.shape) == 4:
                owners, _, owned, _ = out_ref.shape
                block = block.reshape(HALO, owners, owned, channels)
                for frame in range(HALO):
                    out_ref[:, base + frame] = block[frame]
            else:
                out_ref[base : base + HALO] = block.reshape(HALO, ROWS * COLS, channels)
        else:
            out_ref[base : base + HALO] = block


def conv_block(sources, gain, kernel, weight=None, owners=None):
    groups = len(sources)
    ready = tuple(len(source) == 3 for source in sources)
    outcount = HALO * (groups - 1)
    cells, channels = sources[0][0].shape[1:]
    flat_kernel = kernel.reshape(3, 3, 3 * channels, channels)
    block_at = lambda at, *dims: pl.BlockSpec(dims, lambda i: (at,) + (0,) * (len(dims) - 1))
    whole = lambda *dims: pl.BlockSpec(dims, lambda i: (0,) * len(dims))
    operands, specs = [], []
    for source in sources:
        array, dims = (source[2], (HALO, ROWS, COLS, 3 * channels)) if len(source) == 3 else (source[0], (HALO, cells, channels))
        operands.append(array)
        specs.append(block_at(source[1], *dims))
    for source in sources[1:]:
        if len(source) == 3:
            operands.append(source[0])
            specs.append(block_at(source[1], HALO, cells, channels))
    operands += [gain.reshape(1, channels), flat_kernel]
    specs += [whole(1, channels), whole(3, 3, 3 * channels, channels)]
    if weight is not None:
        operands.append(weight)
        specs.append(whole(channels, channels))
    if owners is not None:
        shape = (owners, outcount, cells // owners, channels)
    else:
        shape = (outcount, cells, channels)
    flops = 2 * outcount * cells * 27 * channels * channels
    return pl.pallas_call(
        functools.partial(conv_body, ready, weight is not None),
        grid=(1,),
        in_specs=specs,
        out_specs=whole(*shape),
        out_shape=jax.ShapeDtypeStruct(shape, jnp.bfloat16),
        scratch_shapes=[
            pltpu.VMEM((HALO * groups, ROWS, COLS, 3 * channels), jnp.bfloat16),
            pltpu.VMEM((HALO, cells, channels), jnp.float32),
        ],
        compiler_params=pltpu.CompilerParams(vmem_limit_bytes=VMEM_LIMIT),
        cost_estimate=pl.CostEstimate(
            flops=flops, bytes_accessed=27 * channels * channels * 2, transcendentals=0
        ),
    )(*operands)


def body(frames, gain_one, conv_one, gain_two, conv_two, out_weight):
    local_frames, cells, channels = frames.shape
    members = lax.axis_size("tm")
    owned = cells // members
    assert local_frames == 2 * HALO
    earlier = passed_along(frames[-HALO:], "tm", 1)
    taps = taps_of(frames, gain_one)
    late = conv_block([(frames, 0, taps), (frames, 1, taps)], gain_one, conv_one)
    late_earlier = passed_along(late, "tm", 1)
    early = conv_block([(earlier, 0), (frames, 0, taps)], gain_one, conv_one)
    aligned = owned % 16 == 0
    projected = conv_block(
        [(late_earlier, 0), (early, 0), (late, 0)],
        gain_two,
        conv_two,
        out_weight,
        members if aligned else None,
    )
    if aligned:
        latent = lax.all_to_all(projected, "tm", split_axis=0, concat_axis=0, tiled=True)
    else:
        latent = lax.all_to_all(projected, "tm", split_axis=1, concat_axis=0, tiled=True)
    return latent.reshape(members * local_frames, owned, channels)


def solution(mesh):
    placed = (P("tm", "clip", None), P(), P(), P(), P(), P())
    return jax.shard_map(
        body, mesh=mesh, in_specs=placed, out_specs=P(None, ("clip", "tm"), None), check_vma=False
    )
```

```python
import functools

import jax
import jax.numpy as jnp
from jax import lax
from jax.experimental import pallas as pl
from jax.experimental.pallas import tpu as pltpu
from jax.sharding import PartitionSpec as P

ROWS = 4
COLS = 128
HALO = 2
VMEM_LIMIT = 24 * 1024 * 1024


def passed_along(x, axis, by):
    size = lax.axis_size(axis)
    pairs = [(i, i + by) for i in range(size) if 0 <= i + by < size]
    return lax.ppermute(x, axis, pairs)


def norm_act(x, gain):
    values = x.astype(jnp.float32)
    scale = lax.rsqrt(jnp.mean(values * values, axis=-1, keepdims=True) + 1e-06)
    gated = values * scale * gain
    return gated / (1.0 + jnp.exp(-gated))


def spread(source, frame, row, gain, taps_ref, at):
    channels = source.shape[-1]
    column = lax.broadcasted_iota(jnp.int32, (COLS, channels), 0)
    cells = pl.ds(row * COLS, COLS)
    act = norm_act(source[frame, cells, :], gain)
    left = jnp.where(column == 0, 0.0, pltpu.roll(act, 1, 0))
    right = jnp.where(column == COLS - 1, 0.0, pltpu.roll(act, COLS - 1, 0))
    taps_ref[at, row, :, :channels] = left.astype(jnp.bfloat16)
    taps_ref[at, row, :, channels : 2 * channels] = act.astype(jnp.bfloat16)
    taps_ref[at, row, :, 2 * channels :] = right.astype(jnp.bfloat16)


def taps_body(source, gain_ref, taps_ref):
    gain = gain_ref[...]

    for row in range(ROWS):
        spread(source, 0, row, gain, taps_ref, 0)


def taps_of(x, gain):
    frames, cells, channels = x.shape
    return pl.pallas_call(
        taps_body,
        grid=(frames,),
        in_specs=[
            pl.BlockSpec((1, cells, channels), lambda i: (i, 0, 0)),
            pl.BlockSpec((1, channels), lambda i: (0, 0)),
        ],
        out_specs=pl.BlockSpec((1, ROWS, COLS, 3 * channels), lambda i: (i, 0, 0, 0)),
        out_shape=jax.ShapeDtypeStruct((frames, ROWS, COLS, 3 * channels), jnp.bfloat16),
        compiler_params=pltpu.CompilerParams(vmem_limit_bytes=VMEM_LIMIT),
        cost_estimate=pl.CostEstimate(
            flops=20 * frames * cells * channels, bytes_accessed=8 * frames * cells * channels, transcendentals=0
        ),
    )(x, gain.reshape(1, channels))


def conv_body(ready, project, *refs):
    groups = len(ready)
    sources, refs = refs[:groups], list(refs[groups:])
    residuals = [refs.pop(0) if ready[g] else sources[g] for g in range(1, groups)]
    gain_ref, kernel_ref = refs[:2]
    rest = refs[2:]
    if project:
        weight_ref, rest = rest[0], rest[1:]
    out_ref, taps_ref, sum_ref = rest
    channels = gain_ref.shape[-1]
    gain = gain_ref[...]

    for group, source in enumerate(sources):
        if ready[group]:
            continue

        for frame in range(HALO):
            for row in range(ROWS):
                spread(source, frame, row, gain, taps_ref, HALO * group + frame)

    def tap(frame, row):
        if ready[frame // HALO]:
            return sources[frame // HALO][frame % HALO, row]
        return taps_ref[frame, row]

    for part in range(groups - 1):
        base = HALO * part
        for row in range(ROWS):
            taps = [(a, b) for b in range(3) if 0 <= row + b - 1 < ROWS for a in range(3)]
            window = jnp.concatenate(
                [
                    jnp.concatenate([tap(base + a + f, row + b - 1) for f in range(HALO)], axis=0)
                    for a, b in taps
                ],
                axis=1,
            )
            product = jnp.dot(
                window,
                jnp.concatenate([kernel_ref[a, b] for a, b in taps], axis=0),
                preferred_element_type=jnp.float32,
            ).reshape(HALO, COLS, channels)
            at = slice(row * COLS, (row + 1) * COLS)
            sum_ref[:, at] = product + residuals[part][:, at, :].astype(jnp.float32)
        block = sum_ref[...].astype(jnp.bfloat16)
        if project:
            block = jnp.dot(
                block.reshape(HALO * ROWS * COLS, channels),
                weight_ref[...],
                preferred_element_type=jnp.float32,
            ).astype(jnp.bfloat16)
            if len(out_ref.shape) == 4:
                owners, _, owned, _ = out_ref.shape
                block = block.reshape(HALO, owners, owned, channels)
                for frame in range(HALO):
                    out_ref[:, base + frame] = block[frame]
            else:
                out_ref[base : base + HALO] = block.reshape(HALO, ROWS * COLS, channels)
        else:
            out_ref[base : base + HALO] = block


def conv_block(sources, gain, kernel, weight=None, owners=None):
    groups = len(sources)
    ready = tuple(len(source) == 3 for source in sources)
    outcount = HALO * (groups - 1)
    cells, channels = sources[0][0].shape[1:]
    flat_kernel = kernel.reshape(3, 3, 3 * channels, channels)
    block_at = lambda at, *dims: pl.BlockSpec(dims, lambda i: (at,) + (0,) * (len(dims) - 1))
    whole = lambda *dims: pl.BlockSpec(dims, lambda i: (0,) * len(dims))
    operands, specs = [], []
    for source in sources:
        array, dims = (source[2], (HALO, ROWS, COLS, 3 * channels)) if len(source) == 3 else (source[0], (HALO, cells, channels))
        operands.append(array)
        specs.append(block_at(source[1], *dims))
    for source in sources[1:]:
        if len(source) == 3:
            operands.append(source[0])
            specs.append(block_at(source[1], HALO, cells, channels))
    operands += [gain.reshape(1, channels), flat_kernel]
    specs += [whole(1, channels), whole(3, 3, 3 * channels, channels)]
    if weight is not None:
        operands.append(weight)
        specs.append(whole(channels, channels))
    if owners is not None:
        shape = (owners, outcount, cells // owners, channels)
    else:
        shape = (outcount, cells, channels)
    flops = 2 * outcount * cells * 27 * channels * channels
    return pl.pallas_call(
        functools.partial(conv_body, ready, weight is not None),
        grid=(1,),
        in_specs=specs,
        out_specs=whole(*shape),
        out_shape=jax.ShapeDtypeStruct(shape, jnp.bfloat16),
        scratch_shapes=[
            pltpu.VMEM((HALO * groups, ROWS, COLS, 3 * channels), jnp.bfloat16),
            pltpu.VMEM((HALO, cells, channels), jnp.float32),
        ],
        compiler_params=pltpu.CompilerParams(vmem_limit_bytes=VMEM_LIMIT),
        cost_estimate=pl.CostEstimate(
            flops=flops, bytes_accessed=27 * channels * channels * 2, transcendentals=0
        ),
    )(*operands)


def body(frames, gain_one, conv_one, gain_two, conv_two, out_weight):
    local_frames, cells, channels = frames.shape
    members = lax.axis_size("tm")
    owned = cells // members
    assert local_frames == 2 * HALO
    earlier = passed_along(frames[-HALO:], "tm", 1)
    taps = taps_of(frames, gain_one)
    late = conv_block([(frames, 0, taps), (frames, 1, taps)], gain_one, conv_one)
    late_earlier = passed_along(late, "tm", 1)
    early = conv_block([(earlier, 0), (frames, 0, taps)], gain_one, conv_one)
    aligned = owned % 16 == 0
    projected = conv_block(
        [(late_earlier, 0), (early, 0), (late, 0)],
        gain_two,
        conv_two,
        out_weight,
        members if aligned else None,
    )
    if aligned:
        latent = lax.all_to_all(projected, "tm", split_axis=0, concat_axis=0, tiled=True)
    else:
        latent = lax.all_to_all(projected, "tm", split_axis=1, concat_axis=0, tiled=True)
    return latent.reshape(members * local_frames, owned, channels)


def solution(mesh):
    placed = (P("tm", "clip", None), P(), P(), P(), P(), P())
    return jax.shard_map(
        body, mesh=mesh, in_specs=placed, out_specs=P(None, ("clip", "tm"), None), check_vma=False
    )
```

```python
import functools

import jax
import jax.numpy as jnp
from jax import lax
from jax.experimental import pallas as pl
from jax.experimental.pallas import tpu as pltpu
from jax.sharding import PartitionSpec as P

ROWS = 4
COLS = 128
HALO = 2
VMEM_LIMIT = 24 * 1024 * 1024


def passed_along(x, axis, by):
    size = lax.axis_size(axis)
    pairs = [(i, i + by) for i in range(size) if 0 <= i + by < size]
    return lax.ppermute(x, axis, pairs)


def norm_act(x, gain):
    values = x.astype(jnp.float32)
    scale = lax.rsqrt(jnp.mean(values * values, axis=-1, keepdims=True) + 1e-06)
    gated = values * scale * gain
    return gated / (1.0 + jnp.exp(-gated))


def spread(source, frame, row, gain, taps_ref, at):
    channels = source.shape[-1]
    column = lax.broadcasted_iota(jnp.int32, (COLS, channels), 0)
    cells = pl.ds(row * COLS, COLS)
    act = norm_act(source[frame, cells, :], gain)
    left = jnp.where(column == 0, 0.0, pltpu.roll(act, 1, 0))
    right = jnp.where(column == COLS - 1, 0.0, pltpu.roll(act, COLS - 1, 0))
    taps_ref[at, row, :, :channels] = left.astype(jnp.bfloat16)
    taps_ref[at, row, :, channels : 2 * channels] = act.astype(jnp.bfloat16)
    taps_ref[at, row, :, 2 * channels :] = right.astype(jnp.bfloat16)


def taps_body(source, gain_ref, taps_ref):
    gain = gain_ref[...]

    for row in range(ROWS):
        spread(source, 0, row, gain, taps_ref, 0)


def taps_of(x, gain):
    frames, cells, channels = x.shape
    return pl.pallas_call(
        taps_body,
        grid=(frames,),
        in_specs=[
            pl.BlockSpec((1, cells, channels), lambda i: (i, 0, 0)),
            pl.BlockSpec((1, channels), lambda i: (0, 0)),
        ],
        out_specs=pl.BlockSpec((1, ROWS, COLS, 3 * channels), lambda i: (i, 0, 0, 0)),
        out_shape=jax.ShapeDtypeStruct((frames, ROWS, COLS, 3 * channels), jnp.bfloat16),
        compiler_params=pltpu.CompilerParams(vmem_limit_bytes=VMEM_LIMIT),
        cost_estimate=pl.CostEstimate(
            flops=20 * frames * cells * channels, bytes_accessed=8 * frames * cells * channels, transcendentals=0
        ),
    )(x, gain.reshape(1, channels))


def conv_body(ready, project, onto, *refs):
    groups = len(ready)
    sources, refs = refs[:groups], list(refs[groups:])
    residuals = [refs.pop(0) if ready[g] else sources[g] for g in range(1, groups)]
    gain_ref, kernel_ref = refs[:2]
    rest = refs[2:]
    if project:
        weight_ref, rest = rest[0], rest[1:]
    if onto:
        rest = rest[1:]
    out_ref, taps_ref, sum_ref = rest
    channels = gain_ref.shape[-1]
    gain = gain_ref[...]

    for group, source in enumerate(sources):
        if ready[group]:
            continue

        for frame in range(HALO):
            for row in range(ROWS):
                spread(source, frame, row, gain, taps_ref, HALO * group + frame)

    def tap(frame, row):
        if ready[frame // HALO]:
            return sources[frame // HALO][frame % HALO, row]
        return taps_ref[frame, row]

    for part in range(groups - 1):
        base = HALO * part
        for row in range(ROWS):
            taps = [(a, b) for b in range(3) if 0 <= row + b - 1 < ROWS for a in range(3)]
            window = jnp.concatenate(
                [
                    jnp.concatenate([tap(base + a + f, row + b - 1) for f in range(HALO)], axis=0)
                    for a, b in taps
                ],
                axis=1,
            )
            product = jnp.dot(
                window,
                jnp.concatenate([kernel_ref[a, b] for a, b in taps], axis=0),
                preferred_element_type=jnp.float32,
            ).reshape(HALO, COLS, channels)
            at = slice(row * COLS, (row + 1) * COLS)
            sum_ref[:, at] = product + residuals[part][:, at, :].astype(jnp.float32)
        block = sum_ref[...].astype(jnp.bfloat16)
        if project:
            block = jnp.dot(
                block.reshape(HALO * ROWS * COLS, channels),
                weight_ref[...],
                preferred_element_type=jnp.float32,
            ).astype(jnp.bfloat16)
            if len(out_ref.shape) == 4:
                owners, _, owned, _ = out_ref.shape
                block = block.reshape(HALO, owners, owned, channels)
                for frame in range(HALO):
                    out_ref[:, base + frame] = block[frame]
            else:
                out_ref[base : base + HALO] = block.reshape(HALO, ROWS * COLS, channels)
        else:
            out_ref[base : base + HALO] = block


def conv_block(sources, gain, kernel, weight=None, owners=None, halves=1, half=0, into=None):
    groups = len(sources)
    ready = tuple(len(source) == 3 for source in sources)
    outcount = HALO * (groups - 1)
    cells, channels = sources[0][0].shape[1:]
    flat_kernel = kernel.reshape(3, 3, 3 * channels, channels)
    block_at = lambda at, *dims: pl.BlockSpec(dims, lambda i: (at,) + (0,) * (len(dims) - 1))
    whole = lambda *dims: pl.BlockSpec(dims, lambda i: (0,) * len(dims))
    operands, specs = [], []
    for source in sources:
        array, dims = (source[2], (HALO, ROWS, COLS, 3 * channels)) if len(source) == 3 else (source[0], (HALO, cells, channels))
        operands.append(array)
        specs.append(block_at(source[1], *dims))
    for source in sources[1:]:
        if len(source) == 3:
            operands.append(source[0])
            specs.append(block_at(source[1], HALO, cells, channels))
    operands += [gain.reshape(1, channels), flat_kernel]
    specs += [whole(1, channels), whole(3, 3, 3 * channels, channels)]
    if weight is not None:
        operands.append(weight)
        specs.append(whole(channels, channels))
    if owners is not None:
        block, index = (owners, outcount, cells // owners, channels), (0, half, 0, 0)
        shape = (owners, halves * outcount) + block[2:]
    else:
        block, index = (outcount, cells, channels), (half, 0, 0)
        shape = (halves * outcount,) + block[1:]
    aliases = {}
    if into is not None:
        aliases = {len(operands): 0}
        operands.append(into)
        specs.append(pl.BlockSpec(memory_space=pl.ANY))
    flops = 2 * outcount * cells * 27 * channels * channels
    return pl.pallas_call(
        functools.partial(conv_body, ready, weight is not None, into is not None),
        grid=(1,),
        in_specs=specs,
        out_specs=pl.BlockSpec(block, lambda i: index),
        input_output_aliases=aliases,
        out_shape=jax.ShapeDtypeStruct(shape, jnp.bfloat16),
        scratch_shapes=[
            pltpu.VMEM((HALO * groups, ROWS, COLS, 3 * channels), jnp.bfloat16),
            pltpu.VMEM((HALO, cells, channels), jnp.float32),
        ],
        compiler_params=pltpu.CompilerParams(vmem_limit_bytes=VMEM_LIMIT),
        cost_estimate=pl.CostEstimate(
            flops=flops, bytes_accessed=27 * channels * channels * 2, transcendentals=0
        ),
    )(*operands)


def body(frames, gain_one, conv_one, gain_two, conv_two, out_weight):
    local_frames, cells, channels = frames.shape
    members = lax.axis_size("tm")
    owned = cells // members
    assert local_frames == 2 * HALO
    earlier = passed_along(frames[-HALO:], "tm", 1)
    taps = taps_of(frames, gain_one)
    late = conv_block([(frames, 0, taps), (frames, 1, taps)], gain_one, conv_one)
    late_earlier = passed_along(late, "tm", 1)
    early = conv_block([(earlier, 0), (frames, 0, taps)], gain_one, conv_one)
    aligned = owned % 16 == 0
    owners = members if aligned else None
    projected = conv_block([(early, 0), (late, 0)], gain_two, conv_two, out_weight, owners, halves=2, half=1)
    projected = conv_block(
        [(late_earlier, 0), (early, 0)], gain_two, conv_two, out_weight, owners, halves=2, half=0, into=projected
    )
    if aligned:
        latent = lax.all_to_all(projected, "tm", split_axis=0, concat_axis=0, tiled=True)
    else:
        latent = lax.all_to_all(projected, "tm", split_axis=1, concat_axis=0, tiled=True)
    return latent.reshape(members * local_frames, owned, channels)


def solution(mesh):
    placed = (P("tm", "clip", None), P(), P(), P(), P(), P())
    return jax.shard_map(
        body, mesh=mesh, in_specs=placed, out_specs=P(None, ("clip", "tm"), None), check_vma=False
    )
```

```python
import functools

import jax
import jax.numpy as jnp
from jax import lax
from jax.experimental import pallas as pl
from jax.experimental.pallas import tpu as pltpu
from jax.sharding import PartitionSpec as P

ROWS = 4
COLS = 128
HALO = 2
VMEM_LIMIT = 24 * 1024 * 1024


def passed_along(x, axis, by):
    size = lax.axis_size(axis)
    pairs = [(i, i + by) for i in range(size) if 0 <= i + by < size]
    return lax.ppermute(x, axis, pairs)


def norm_act(x, gain):
    values = x.astype(jnp.float32)
    scale = lax.rsqrt(jnp.mean(values * values, axis=-1, keepdims=True) + 1e-06)
    gated = values * scale * gain
    return gated / (1.0 + jnp.exp(-gated))


def spread(source, frame, row, gain, taps_ref, at):
    channels = source.shape[-1]
    column = lax.broadcasted_iota(jnp.int32, (COLS, channels), 0)
    cells = pl.ds(row * COLS, COLS)
    act = norm_act(source[frame, cells, :], gain)
    left = jnp.where(column == 0, 0.0, pltpu.roll(act, 1, 0))
    right = jnp.where(column == COLS - 1, 0.0, pltpu.roll(act, COLS - 1, 0))
    taps_ref[at, row, :, :channels] = left.astype(jnp.bfloat16)
    taps_ref[at, row, :, channels : 2 * channels] = act.astype(jnp.bfloat16)
    taps_ref[at, row, :, 2 * channels :] = right.astype(jnp.bfloat16)


def taps_body(source, gain_ref, taps_ref):
    gain = gain_ref[...]

    for row in range(ROWS):
        spread(source, 0, row, gain, taps_ref, 0)


def taps_of(x, gain):
    frames, cells, channels = x.shape
    return pl.pallas_call(
        taps_body,
        grid=(frames,),
        in_specs=[
            pl.BlockSpec((1, cells, channels), lambda i: (i, 0, 0)),
            pl.BlockSpec((1, channels), lambda i: (0, 0)),
        ],
        out_specs=pl.BlockSpec((1, ROWS, COLS, 3 * channels), lambda i: (i, 0, 0, 0)),
        out_shape=jax.ShapeDtypeStruct((frames, ROWS, COLS, 3 * channels), jnp.bfloat16),
        compiler_params=pltpu.CompilerParams(vmem_limit_bytes=VMEM_LIMIT),
        cost_estimate=pl.CostEstimate(
            flops=20 * frames * cells * channels, bytes_accessed=8 * frames * cells * channels, transcendentals=0
        ),
    )(x, gain.reshape(1, channels))


def copy_body(source, out_ref):
    out_ref[...] = source[...]


def last_frames(x):
    frames, cells, channels = x.shape
    return pl.pallas_call(
        copy_body,
        grid=(1,),
        in_specs=[pl.BlockSpec((HALO, cells, channels), lambda i: (frames // HALO - 1, 0, 0))],
        out_specs=pl.BlockSpec((HALO, cells, channels), lambda i: (0, 0, 0)),
        out_shape=jax.ShapeDtypeStruct((HALO, cells, channels), x.dtype),
        compiler_params=pltpu.CompilerParams(vmem_limit_bytes=VMEM_LIMIT),
        cost_estimate=pl.CostEstimate(
            flops=HALO * cells * channels, bytes_accessed=4 * HALO * cells * channels, transcendentals=0
        ),
    )(x)


def conv_body(ready, project, onto, *refs):
    groups = len(ready)
    sources, refs = refs[:groups], list(refs[groups:])
    residuals = [refs.pop(0) if ready[g] else sources[g] for g in range(1, groups)]
    gain_ref, kernel_ref = refs[:2]
    rest = refs[2:]
    if project:
        weight_ref, rest = rest[0], rest[1:]
    if onto:
        rest = rest[1:]
    out_ref, taps_ref, sum_ref = rest
    channels = gain_ref.shape[-1]
    gain = gain_ref[...]

    for group, source in enumerate(sources):
        if ready[group]:
            continue

        for frame in range(HALO):
            for row in range(ROWS):
                spread(source, frame, row, gain, taps_ref, HALO * group + frame)

    def tap(frame, row):
        if ready[frame // HALO]:
            return sources[frame // HALO][frame % HALO, row]
        return taps_ref[frame, row]

    for part in range(groups - 1):
        base = HALO * part
        for row in range(ROWS):
            taps = [(a, b) for b in range(3) if 0 <= row + b - 1 < ROWS for a in range(3)]
            window = jnp.concatenate(
                [
                    jnp.concatenate([tap(base + a + f, row + b - 1) for f in range(HALO)], axis=0)
                    for a, b in taps
                ],
                axis=1,
            )
            product = jnp.dot(
                window,
                jnp.concatenate([kernel_ref[a, b] for a, b in taps], axis=0),
                preferred_element_type=jnp.float32,
            ).reshape(HALO, COLS, channels)
            at = slice(row * COLS, (row + 1) * COLS)
            sum_ref[:, at] = product + residuals[part][:, at, :].astype(jnp.float32)
        block = sum_ref[...].astype(jnp.bfloat16)
        if project:
            block = jnp.dot(
                block.reshape(HALO * ROWS * COLS, channels),
                weight_ref[...],
                preferred_element_type=jnp.float32,
            ).astype(jnp.bfloat16)
            if len(out_ref.shape) == 4:
                owners, _, owned, _ = out_ref.shape
                block = block.reshape(HALO, owners, owned, channels)
                for frame in range(HALO):
                    out_ref[:, base + frame] = block[frame]
            else:
                out_ref[base : base + HALO] = block.reshape(HALO, ROWS * COLS, channels)
        else:
            out_ref[base : base + HALO] = block


def conv_block(sources, gain, kernel, weight=None, owners=None, halves=1, half=0, into=None):
    groups = len(sources)
    ready = tuple(len(source) == 3 for source in sources)
    outcount = HALO * (groups - 1)
    cells, channels = sources[0][0].shape[1:]
    flat_kernel = kernel.reshape(3, 3, 3 * channels, channels)
    block_at = lambda at, *dims: pl.BlockSpec(dims, lambda i: (at,) + (0,) * (len(dims) - 1))
    whole = lambda *dims: pl.BlockSpec(dims, lambda i: (0,) * len(dims))
    operands, specs = [], []
    for source in sources:
        array, dims = (source[2], (HALO, ROWS, COLS, 3 * channels)) if len(source) == 3 else (source[0], (HALO, cells, channels))
        operands.append(array)
        specs.append(block_at(source[1], *dims))
    for source in sources[1:]:
        if len(source) == 3:
            operands.append(source[0])
            specs.append(block_at(source[1], HALO, cells, channels))
    operands += [gain.reshape(1, channels), flat_kernel]
    specs += [whole(1, channels), whole(3, 3, 3 * channels, channels)]
    if weight is not None:
        operands.append(weight)
        specs.append(whole(channels, channels))
    if owners is not None:
        block, index = (owners, outcount, cells // owners, channels), (0, half, 0, 0)
        shape = (owners, halves * outcount) + block[2:]
    else:
        block, index = (outcount, cells, channels), (half, 0, 0)
        shape = (halves * outcount,) + block[1:]
    aliases = {}
    if into is not None:
        aliases = {len(operands): 0}
        operands.append(into)
        specs.append(pl.BlockSpec(memory_space=pl.ANY))
    flops = 2 * outcount * cells * 27 * channels * channels
    return pl.pallas_call(
        functools.partial(conv_body, ready, weight is not None, into is not None),
        grid=(1,),
        in_specs=specs,
        out_specs=pl.BlockSpec(block, lambda i: index),
        input_output_aliases=aliases,
        out_shape=jax.ShapeDtypeStruct(shape, jnp.bfloat16),
        scratch_shapes=[
            pltpu.VMEM((HALO * groups, ROWS, COLS, 3 * channels), jnp.bfloat16),
            pltpu.VMEM((HALO, cells, channels), jnp.float32),
        ],
        compiler_params=pltpu.CompilerParams(vmem_limit_bytes=VMEM_LIMIT),
        cost_estimate=pl.CostEstimate(
            flops=flops, bytes_accessed=27 * channels * channels * 2, transcendentals=0
        ),
    )(*operands)


def body(frames, gain_one, conv_one, gain_two, conv_two, out_weight):
    local_frames, cells, channels = frames.shape
    members = lax.axis_size("tm")
    owned = cells // members
    assert local_frames == 2 * HALO
    earlier = passed_along(last_frames(frames), "tm", 1)
    taps = taps_of(frames, gain_one)
    late = conv_block([(frames, 0, taps), (frames, 1, taps)], gain_one, conv_one)
    late_earlier = passed_along(late, "tm", 1)
    early = conv_block([(earlier, 0), (frames, 0, taps)], gain_one, conv_one)
    aligned = owned % 16 == 0
    owners = members if aligned else None
    projected = conv_block([(early, 0), (late, 0)], gain_two, conv_two, out_weight, owners, halves=2, half=1)
    projected = conv_block(
        [(late_earlier, 0), (early, 0)], gain_two, conv_two, out_weight, owners, halves=2, half=0, into=projected
    )
    if aligned:
        latent = lax.all_to_all(projected, "tm", split_axis=0, concat_axis=0, tiled=True)
    else:
        latent = lax.all_to_all(projected, "tm", split_axis=1, concat_axis=0, tiled=True)
    return latent.reshape(members * local_frames, owned, channels)


def solution(mesh):
    placed = (P("tm", "clip", None), P(), P(), P(), P(), P())
    return jax.shard_map(
        body, mesh=mesh, in_specs=placed, out_specs=P(None, ("clip", "tm"), None), check_vma=False
    )
```

```python
import functools

import jax
import jax.numpy as jnp
from jax import lax
from jax.experimental import pallas as pl
from jax.experimental.pallas import tpu as pltpu
from jax.sharding import PartitionSpec as P

ROWS = 4
COLS = 128
HALO = 2
VMEM_LIMIT = 24 * 1024 * 1024


def passed_along(x, axis, by):
    size = lax.axis_size(axis)
    pairs = [(i, i + by) for i in range(size) if 0 <= i + by < size]
    return lax.ppermute(x, axis, pairs)


def norm_act(x, gain):
    values = x.astype(jnp.float32)
    scale = lax.rsqrt(jnp.mean(values * values, axis=-1, keepdims=True) + 1e-06)
    gated = values * scale * gain
    return gated / (1.0 + jnp.exp(-gated))


def spread(source, frame, row, gain, taps_ref, at):
    channels = source.shape[-1]
    column = lax.broadcasted_iota(jnp.int32, (COLS, channels), 0)
    cells = pl.ds(row * COLS, COLS)
    act = norm_act(source[frame, cells, :], gain)
    left = jnp.where(column == 0, 0.0, pltpu.roll(act, 1, 0))
    right = jnp.where(column == COLS - 1, 0.0, pltpu.roll(act, COLS - 1, 0))
    taps_ref[at, row, :, :channels] = left.astype(jnp.bfloat16)
    taps_ref[at, row, :, channels : 2 * channels] = act.astype(jnp.bfloat16)
    taps_ref[at, row, :, 2 * channels :] = right.astype(jnp.bfloat16)


def taps_body(source, gain_ref, taps_ref):
    gain = gain_ref[...]

    for row in range(ROWS):
        spread(source, 0, row, gain, taps_ref, 0)


def taps_of(x, gain):
    frames, cells, channels = x.shape
    return pl.pallas_call(
        taps_body,
        grid=(frames,),
        in_specs=[
            pl.BlockSpec((1, cells, channels), lambda i: (i, 0, 0)),
            pl.BlockSpec((1, channels), lambda i: (0, 0)),
        ],
        out_specs=pl.BlockSpec((1, ROWS, COLS, 3 * channels), lambda i: (i, 0, 0, 0)),
        out_shape=jax.ShapeDtypeStruct((frames, ROWS, COLS, 3 * channels), jnp.bfloat16),
        compiler_params=pltpu.CompilerParams(vmem_limit_bytes=VMEM_LIMIT),
        cost_estimate=pl.CostEstimate(
            flops=20 * frames * cells * channels, bytes_accessed=8 * frames * cells * channels, transcendentals=0
        ),
    )(x, gain.reshape(1, channels))


def copy_body(source, gain_ref, out_ref, gain_out_ref):
    out_ref[...] = source[...]
    gain_out_ref[...] = gain_ref[...]


def last_frames(x, gain):
    frames, cells, channels = x.shape
    return pl.pallas_call(
        copy_body,
        grid=(1,),
        in_specs=[
            pl.BlockSpec((HALO, cells, channels), lambda i: (frames // HALO - 1, 0, 0)),
            pl.BlockSpec((1, channels), lambda i: (0, 0)),
        ],
        out_specs=[
            pl.BlockSpec((HALO, cells, channels), lambda i: (0, 0, 0)),
            pl.BlockSpec((1, channels), lambda i: (0, 0)),
        ],
        out_shape=[
            jax.ShapeDtypeStruct((HALO, cells, channels), x.dtype),
            jax.ShapeDtypeStruct((1, channels), gain.dtype),
        ],
        compiler_params=pltpu.CompilerParams(vmem_limit_bytes=VMEM_LIMIT),
        cost_estimate=pl.CostEstimate(
            flops=HALO * cells * channels, bytes_accessed=4 * HALO * cells * channels, transcendentals=0
        ),
    )(x, gain.reshape(1, channels))


def conv_body(ready, project, onto, *refs):
    groups = len(ready)
    sources, refs = refs[:groups], list(refs[groups:])
    residuals = [refs.pop(0) if ready[g] else sources[g] for g in range(1, groups)]
    gain_ref, kernel_ref = refs[:2]
    rest = refs[2:]
    if project:
        weight_ref, rest = rest[0], rest[1:]
    if onto:
        rest = rest[1:]
    out_ref, taps_ref, sum_ref = rest
    channels = gain_ref.shape[-1]
    gain = gain_ref[...]

    for group, source in enumerate(sources):
        if ready[group]:
            continue

        for frame in range(HALO):
            for row in range(ROWS):
                spread(source, frame, row, gain, taps_ref, HALO * group + frame)

    def tap(frame, row):
        if ready[frame // HALO]:
            return sources[frame // HALO][frame % HALO, row]
        return taps_ref[frame, row]

    for part in range(groups - 1):
        base = HALO * part
        for row in range(ROWS):
            taps = [(a, b) for b in range(3) if 0 <= row + b - 1 < ROWS for a in range(3)]
            window = jnp.concatenate(
                [
                    jnp.concatenate([tap(base + a + f, row + b - 1) for f in range(HALO)], axis=0)
                    for a, b in taps
                ],
                axis=1,
            )
            product = jnp.dot(
                window,
                jnp.concatenate([kernel_ref[a, b] for a, b in taps], axis=0),
                preferred_element_type=jnp.float32,
            ).reshape(HALO, COLS, channels)
            at = slice(row * COLS, (row + 1) * COLS)
            sum_ref[:, at] = product + residuals[part][:, at, :].astype(jnp.float32)
        block = sum_ref[...].astype(jnp.bfloat16)
        if project:
            block = jnp.dot(
                block.reshape(HALO * ROWS * COLS, channels),
                weight_ref[...],
                preferred_element_type=jnp.float32,
            ).astype(jnp.bfloat16)
            if len(out_ref.shape) == 4:
                owners, _, owned, _ = out_ref.shape
                block = block.reshape(HALO, owners, owned, channels)
                for frame in range(HALO):
                    out_ref[:, base + frame] = block[frame]
            else:
                out_ref[base : base + HALO] = block.reshape(HALO, ROWS * COLS, channels)
        else:
            out_ref[base : base + HALO] = block


def conv_block(sources, gain, kernel, weight=None, owners=None, halves=1, half=0, into=None):
    groups = len(sources)
    ready = tuple(len(source) == 3 for source in sources)
    outcount = HALO * (groups - 1)
    cells, channels = sources[0][0].shape[1:]
    flat_kernel = kernel.reshape(3, 3, 3 * channels, channels)
    block_at = lambda at, *dims: pl.BlockSpec(dims, lambda i: (at,) + (0,) * (len(dims) - 1))
    whole = lambda *dims: pl.BlockSpec(dims, lambda i: (0,) * len(dims))
    operands, specs = [], []
    for source in sources:
        array, dims = (source[2], (HALO, ROWS, COLS, 3 * channels)) if len(source) == 3 else (source[0], (HALO, cells, channels))
        operands.append(array)
        specs.append(block_at(source[1], *dims))
    for source in sources[1:]:
        if len(source) == 3:
            operands.append(source[0])
            specs.append(block_at(source[1], HALO, cells, channels))
    operands += [gain.reshape(1, channels), flat_kernel]
    specs += [whole(1, channels), whole(3, 3, 3 * channels, channels)]
    if weight is not None:
        operands.append(weight)
        specs.append(whole(channels, channels))
    if owners is not None:
        block, index = (owners, outcount, cells // owners, channels), (0, half, 0, 0)
        shape = (owners, halves * outcount) + block[2:]
    else:
        block, index = (outcount, cells, channels), (half, 0, 0)
        shape = (halves * outcount,) + block[1:]
    aliases = {}
    if into is not None:
        aliases = {len(operands): 0}
        operands.append(into)
        specs.append(pl.BlockSpec(memory_space=pl.ANY))
    flops = 2 * outcount * cells * 27 * channels * channels
    return pl.pallas_call(
        functools.partial(conv_body, ready, weight is not None, into is not None),
        grid=(1,),
        in_specs=specs,
        out_specs=pl.BlockSpec(block, lambda i: index),
        input_output_aliases=aliases,
        out_shape=jax.ShapeDtypeStruct(shape, jnp.bfloat16),
        scratch_shapes=[
            pltpu.VMEM((HALO * groups, ROWS, COLS, 3 * channels), jnp.bfloat16),
            pltpu.VMEM((HALO, cells, channels), jnp.float32),
        ],
        compiler_params=pltpu.CompilerParams(vmem_limit_bytes=VMEM_LIMIT),
        cost_estimate=pl.CostEstimate(
            flops=flops, bytes_accessed=27 * channels * channels * 2, transcendentals=0
        ),
    )(*operands)


def body(frames, gain_one, conv_one, gain_two, conv_two, out_weight):
    local_frames, cells, channels = frames.shape
    members = lax.axis_size("tm")
    owned = cells // members
    assert local_frames == 2 * HALO
    tail, gain_one = last_frames(frames, gain_one)
    earlier = passed_along(tail, "tm", 1)
    taps = taps_of(frames, gain_one)
    late = conv_block([(frames, 0, taps), (frames, 1, taps)], gain_one, conv_one)
    late_earlier = passed_along(late, "tm", 1)
    early = conv_block([(earlier, 0), (frames, 0, taps)], gain_one, conv_one)
    aligned = owned % 16 == 0
    owners = members if aligned else None
    projected = conv_block([(early, 0), (late, 0)], gain_two, conv_two, out_weight, owners, halves=2, half=1)
    projected = conv_block(
        [(late_earlier, 0), (early, 0)], gain_two, conv_two, out_weight, owners, halves=2, half=0, into=projected
    )
    if aligned:
        latent = lax.all_to_all(projected, "tm", split_axis=0, concat_axis=0, tiled=True)
    else:
        latent = lax.all_to_all(projected, "tm", split_axis=1, concat_axis=0, tiled=True)
    return latent.reshape(members * local_frames, owned, channels)


def solution(mesh):
    placed = (P("tm", "clip", None), P(), P(), P(), P(), P())
    return jax.shard_map(
        body, mesh=mesh, in_specs=placed, out_specs=P(None, ("clip", "tm"), None), check_vma=False
    )
```
